32 devices in a mesh: dp: 2 (over x), fsdp: 4 (over z), tp: 4 (over y, core).
Axes of the slice: x: 2, y: 2, z: 4, core: 2. Of those that a mesh axis runs over, the one named last changes fastest.
Arguments:
- hidden: bfloat16 [16384, 768], P(('dp', 'fsdp', 'tp')), parts along dimension 0
- w_head: bfloat16 [768, 50304], P('fsdp', 'tp')
- labels: int32 [16384], P(('dp', 'fsdp', 'tp')), parts along dimension 0
Outputs:
- output 1: float32 [2], P('dp'), parts along dimension 0
- output 2: bfloat16 [16384, 768], P(('dp', 'fsdp', 'tp')), parts along dimension 0
- output 3: bfloat16 [1536, 50304], P(('dp', 'fsdp'), 'tp'), parts along dimension 0
There are 2 independent parts. The reference program is written for one: setup_inputs(seed, part) draws one part's arguments, and reference() takes and returns one part's arrays. A program takes and returns all parts, laid end to end along the dimension named above; an argument that names none is the same for every part.
All inputs are finite; a program needn't handle non-finite values.
Results may differ from the reference program's by a relative error of at most 0.001.
Values are sent between devices in bfloat16 or wider.
A program may use at most 1 GiB of HBM per device.

```python
import jax
import jax.numpy as jnp
from jax import lax

HIDDEN = 768
VOCAB = 50304
TOKENS = 8192
ROW_BLOCK = 32
COL_ROWS = 256
VOCAB_SPLIT = 16


def setup_inputs(seed: int = 0, part: int = 0) -> dict:
    base_key = jax.random.key(seed)
    key_head, key_data = jax.random.split(base_key)
    part_key = jax.random.fold_in(key_data, part)
    key_hidden, key_labels = jax.random.split(part_key)
    hidden = jax.random.normal(key_hidden, (TOKENS, HIDDEN), jnp.float32)
    w_head = jax.random.normal(key_head, (HIDDEN, VOCAB), jnp.float32) * (2.0 * HIDDEN ** -0.5)
    labels = jax.random.randint(key_labels, (TOKENS,), 0, VOCAB, jnp.int32)
    labels = labels.at[0].set(VOCAB - 1).at[1].set(0)
    return {"hidden": hidden.astype(jnp.bfloat16), "w_head": w_head.astype(jnp.bfloat16), "labels": labels}


def reference(hidden, w_head, labels):
    inv_tokens = 1.0 / TOKENS
    vocab_ids = jnp.arange(VOCAB, dtype=jnp.int32)
    x_blocks = hidden.reshape(TOKENS // ROW_BLOCK, ROW_BLOCK, HIDDEN)
    lab_blocks = labels.reshape(TOKENS // ROW_BLOCK, ROW_BLOCK)

    def row_pass(block):
        x_block, lab_block = block
        logits = jnp.dot(x_block, w_head, preferred_element_type=jnp.float32)
        row_max = jnp.max(logits, axis=1)
        exp_rows = jnp.exp(logits - row_max[:, None])
        row_sum = jnp.sum(exp_rows, axis=1)
        onehot = vocab_ids[None, :] == lab_block[:, None]
        target = jnp.sum(jnp.where(onehot, logits, 0.0), axis=1)
        tok_loss = row_max + jnp.log(row_sum) - target
        prob_rows = exp_rows / row_sum[:, None]
        grad_logits = (jnp.where(onehot, prob_rows - 1.0, prob_rows) * inv_tokens).astype(jnp.bfloat16)
        d_rows = jnp.dot(grad_logits, w_head.T, preferred_element_type=jnp.float32).astype(jnp.bfloat16)
        return tok_loss, row_max, row_sum, d_rows

    tok_loss, row_max, row_sum, d_rows = lax.map(row_pass, (x_blocks, lab_blocks))
    mean_loss = jnp.mean(tok_loss).reshape(1)
    d_hidden = d_rows.reshape(TOKENS, HIDDEN)

    col_width = VOCAB // VOCAB_SPLIT
    row_count = TOKENS // COL_ROWS
    x_cols = hidden.reshape(row_count, COL_ROWS, HIDDEN)
    lab_cols = labels.reshape(row_count, COL_ROWS)
    max_cols = row_max.reshape(row_count, COL_ROWS)
    sum_cols = row_sum.reshape(row_count, COL_ROWS)
    col_ids = jnp.arange(col_width, dtype=jnp.int32)

    def col_pass(col_index):
        col_start = col_index * col_width
        w_cols = lax.dynamic_slice_in_dim(w_head, col_start, col_width, axis=1)

        def row_step(grad_acc, block):
            x_block, lab_block, max_block, sum_block = block
            logits = jnp.dot(x_block, w_cols, preferred_element_type=jnp.float32)
            onehot = (col_ids + col_start)[None, :] == lab_block[:, None]
            prob_rows = jnp.exp(logits - max_block[:, None]) / sum_block[:, None]
            grad_logits = (jnp.where(onehot, prob_rows - 1.0, prob_rows) * inv_tokens).astype(jnp.bfloat16)
            grad_acc = grad_acc + jnp.dot(x_block.T, grad_logits, preferred_element_type=jnp.float32)
            return grad_acc, None

        grad_init = jnp.zeros((HIDDEN, col_width), jnp.float32)
        grad_acc, unused_out = lax.scan(row_step, grad_init, (x_cols, lab_cols, max_cols, sum_cols))
        return grad_acc.astype(jnp.bfloat16)

    d_blocks = lax.map(col_pass, jnp.arange(VOCAB_SPLIT, dtype=jnp.int32))
    d_w_head = jnp.transpose(d_blocks, (1, 0, 2)).reshape(HIDDEN, VOCAB)
    return mean_loss, d_hidden, d_w_head
```

```python
import functools

import jax
import jax.numpy as jnp
from jax import lax
from jax.experimental import pallas as pl
from jax.experimental.pallas import tpu as pltpu
from jax.sharding import PartitionSpec as P


LANES = 128
MESH = pl.DeviceIdType.MESH
NEG = -3.0e38
VMEM_LIMIT = 60 * 1024 * 1024
CHUNKS = 4
STATS = 4


def _ceil_to(n, m):
    return -(-n // m) * m


def _rows_to_cols(ref):
    cols = [jnp.concatenate([ref[b]] * (LANES // ref.shape[1]), axis=0).T for b in range(ref.shape[0])]
    return jnp.concatenate(cols, axis=0)


def _tiles(vp):
    width = vp // 4 // 256 * 256
    edges = [0, width, 2 * width, 3 * width, vp]
    return list(zip(edges[:-1], edges[1:]))


def _logits_kernel(vp, valid_ref, x_ref, w_ref, lab_ref, z_ref, st_ref, xt_ref, m_ref, s_ref, t_ref, l_ref):
    rows, _ = x_ref.shape[1:]
    valid = valid_ref[0]
    x = x_ref[0]
    lane = lax.broadcasted_iota(jnp.int32, (rows, LANES), 1)
    l_ref[...] = _rows_to_cols(lab_ref)[:, 0:1].astype(jnp.int32) - lane
    m_ref[...] = jnp.full((rows, LANES), NEG, jnp.float32)
    s_ref[...] = jnp.zeros((rows, LANES), jnp.float32)
    t_ref[...] = jnp.zeros((rows, LANES), jnp.float32)
    step = 32

    def stats(c0, c1):
        for r in range(0, rows, step):
            sl = slice(r, r + step)
            zs = [z_ref[0, sl, k:k + LANES] for k in range(c0, c1, LANES)]
            off = l_ref[sl, :]
            t = t_ref[sl, :]
            m_old = m_ref[sl, :]
            m = m_old
            for zk, k in zip(zs, range(c0, c1, LANES)):
                t = t + jnp.where(off == k, zk, 0.0)
                m = jnp.maximum(m, zk)
            s = s_ref[sl, :] * jnp.exp(m_old - m)
            for zk in zs:
                s = s + jnp.exp(zk - m)
            m_ref[sl, :] = m
            s_ref[sl, :] = s
            t_ref[sl, :] = t

    before = None
    for c0, c1 in _tiles(vp):
        z = jnp.dot(x, w_ref[:, c0:c1], preferred_element_type=jnp.float32)
        if c1 == vp:
            edge = (vp - 2 * LANES - c0) // LANES * LANES
            z_ref[0, :, c0:c0 + edge] = z[:, :edge]
            for k in range(edge, c1 - c0, LANES):
                z_ref[0, :, c0 + k:c0 + k + LANES] = jnp.where(lane < valid - (c0 + k), z[:, k:k + LANES], NEG)
        else:
            z_ref[0, :, c0:c1] = z
        if before is not None:
            stats(*before)
        before = (c0, c1)
    xt_ref[...] = x.T
    stats(*before)
    m = m_ref[...]
    m_row = jnp.max(m, axis=1, keepdims=True)
    s_row = jnp.sum(s_ref[...] * jnp.exp(m - m_row), axis=1, keepdims=True)
    t_row = jnp.sum(t_ref[...], axis=1, keepdims=True)
    packed = jnp.where(lane == 0, m_row, jnp.where(lane == 1, s_row, t_row))
    st_ref[0] = packed.T[0:STATS, :]


def _grad_kernel(v0, inv_tokens, ids_ref, z_ref, w_ref, st_ref, lab_ref, *rest):
    g0_ref, g1_ref, keep_ref, send_ref = rest[-4:]
    blocks, sub, vp = z_ref.shape
    rows = blocks * sub
    st = _rows_to_cols(st_ref)
    m_row = st[:, 0:1]
    scale = st[:, 1:2] * inv_tokens
    lab_off = _rows_to_cols(lab_ref)[:, 0:1].astype(jnp.int32) - lax.broadcasted_iota(jnp.int32, (rows, LANES), 1)
    dims = (((1,), (1,)), ((), ()))

    for k in range(0, vp, LANES):
        p = jnp.exp(z_ref[:, :, k:k + LANES].reshape(rows, LANES) - m_row) * scale
        g = jnp.where(lab_off == k, p - inv_tokens, p).astype(jnp.bfloat16).reshape(blocks, sub, LANES)
        if k < v0:
            g0_ref[:, :, k:k + LANES] = g
        else:
            g1_ref[:, :, k - v0:k - v0 + LANES] = g
    total = lax.dot_general(g0_ref[...].reshape(rows, v0), w_ref[:, :v0], dims, preferred_element_type=jnp.float32)
    total = total + lax.dot_general(g1_ref[...].reshape(rows, vp - v0), w_ref[:, v0:], dims, preferred_element_type=jnp.float32)
    total = total.reshape(keep_ref.shape)
    i = pl.program_id(0)

    @pl.when(i < 2)
    def _():
        send_ref[...] = total

    @pl.when(i >= 2)
    def _():
        keep_ref[...] = total


def _dw_kernel(steps, xt_ref, g_ref, o_ref, acc_ref):
    k = pl.program_id(0)

    @pl.when(k == 0)
    def _():
        acc_ref[...] = jnp.zeros_like(acc_ref)

    g = g_ref[...].reshape(xt_ref.shape[1], g_ref.shape[2])
    acc_ref[...] += jnp.dot(xt_ref[...], g, preferred_element_type=jnp.float32)

    @pl.when(k == steps - 1)
    def _():
        o_ref[...] = acc_ref[...].astype(o_ref.dtype)


def _gather_kernel(w_ref, x_ref, l_ref, wf_ref, xf_ref, lf_ref, w_buf, x_buf, l_buf, loc,
                   w_s, w_r, wx_s, wx_r, x_s, x_r, y_s, y_r, c_s, c_r, l_s, l_r):
    n_z, n_tp = 4, 4
    n = n_z * n_tp
    dp, zi, tp = lax.axis_index("dp"), lax.axis_index("fsdp"), lax.axis_index("tp")
    w_rows = w_ref.shape[0]
    half = w_rows // 2
    vp = wf_ref.shape[1]
    mine = tp * n_z + zi

    def dev(p):
        return (dp, lax.rem(p, n_z), lax.div(p, n_z))

    peers = [dev(lax.rem(mine + o, n)) for o in range(n)]
    y_tp, c_tp = lax.rem(tp + 2, n_tp), tp + 1 - 2 * lax.rem(tp, 2)
    y_dev, c_dev, x_dev = (dp, zi, y_tp), (dp, zi, c_tp), (1 - dp, zi, tp)
    near, far, third = zi + 1 - 2 * lax.rem(zi, 2), lax.rem(zi + 2, n_z), n_z - 1 - zi
    z_owner = [zi, near, far, third]
    near_dev, far_dev = (dp, near, tp), (dp, far, tp)

    barrier = pltpu.get_barrier_semaphore()
    for d in peers[1:] + [x_dev]:
        pl.semaphore_signal(barrier, inc=1, device_id=d, device_id_type=MESH)
    pl.semaphore_wait(barrier, n)

    def remote(src, dst, s_sem, r_sem, d):
        return pltpu.make_async_remote_copy(src, dst, s_sem, r_sem, device_id=d, device_id_type=MESH)

    def w_half(owner, part):
        return wf_ref.at[pl.ds(pl.multiple_of(owner * w_rows + part * half, 8), half), :]

    def w_cols(z):
        return pl.ds(pl.multiple_of(z * vp, LANES), vp)

    sends = []

    def go(copy):
        copy.start()
        sends.append(copy)
        return copy

    load_x = pltpu.make_async_copy(x_ref, x_buf, loc.at[0])
    load_w = pltpu.make_async_copy(w_ref.at[:, w_cols(zi)], w_buf, loc.at[1])
    load_l = pltpu.make_async_copy(l_ref, l_buf, loc.at[2])
    load_x.start()
    load_w.start()
    load_l.start()
    x_in = [None] * n_z
    x_in[2] = go(remote(x_ref, xf_ref.at[mine], x_s.at[2], x_r.at[2], far_dev))
    x_in[1] = go(remote(x_ref, xf_ref.at[mine], x_s.at[1], x_r.at[1], near_dev))
    y_in = [go(remote(x_ref, xf_ref.at[mine], y_s.at[0], y_r.at[0], y_dev))]
    c_in = [go(remote(x_ref, xf_ref.at[mine], c_s.at[0], c_r.at[0], c_dev))]
    l_in = [go(remote(l_ref, lf_ref.at[mine], l_s.at[o], l_r.at[o], peers[o])) for o in range(1, n)]
    w_in = [None] * n_z
    for s in (2, 1, 3):
        src = w_ref.at[pl.ds(pl.multiple_of(dp * half, 8), half), w_cols(lax.rem(zi + s, n_z))]
        w_in[s] = go(remote(src, w_half(zi, dp), w_s.at[s], w_r.at[s], (dp, lax.rem(zi + s, n_z), tp)))
    load_x.wait()
    load_w.wait()
    load_l.wait()
    store_x = pltpu.make_async_copy(x_buf, xf_ref.at[mine], loc.at[0])
    store_w = pltpu.make_async_copy(w_buf, wf_ref.at[pl.ds(pl.multiple_of(zi * w_rows, 8), w_rows), :], loc.at[1])
    store_l = pltpu.make_async_copy(l_buf, lf_ref.at[mine], loc.at[2])
    store_x.start()
    store_w.start()
    store_l.start()
    wx_in = []
    for j in (2, 1, 3):
        x_in[j].wait_recv()
        blk = xf_ref.at[tp * n_z + z_owner[j]]
        if j == 2:
            x_in[3] = go(remote(blk, blk, x_s.at[3], x_r.at[3], near_dev))
        y_in.append(go(remote(blk, blk, y_s.at[j], y_r.at[j], y_dev)))
        c_in.append(go(remote(blk, blk, c_s.at[j], c_r.at[j], c_dev)))
        if j == 3:
            break
        w_in[j].wait_recv()
        part = w_half(lax.rem(zi + n_z - j, n_z), dp)
        wx_in.append(go(remote(part, part, wx_s.at[j], wx_r.at[j], x_dev)))
    w_in[3].wait_recv()
    part = w_half(lax.rem(zi + 1, n_z), dp)
    wx_in.append(go(remote(part, part, wx_s.at[3], wx_r.at[3], x_dev)))
    for copy, j in zip(y_in, (0, 2, 1, 3)):
        copy.wait_recv()
        blk = xf_ref.at[y_tp * n_z + z_owner[j]]
        c_in.append(go(remote(blk, blk, c_s.at[n_z + j], c_r.at[n_z + j], c_dev)))
    for copy in wx_in + c_in + l_in:
        copy.wait_recv()
    for copy in sends:
        copy.wait_send()
    store_x.wait()
    store_w.wait()
    store_l.wait()


def _gather_call(w_pad, hidden, labels, vp, n_blocks):
    w_rows = w_pad.shape[0]
    rows, hid = hidden.shape
    dma = pltpu.SemaphoreType.DMA
    return pl.pallas_call(
        _gather_kernel,
        in_specs=[pl.BlockSpec(memory_space=pl.ANY)] * 3,
        out_specs=[pl.BlockSpec(memory_space=pl.ANY)] * 3,
        out_shape=[
            jax.ShapeDtypeStruct((hid, vp), jnp.bfloat16),
            jax.ShapeDtypeStruct((n_blocks, rows, hid), jnp.bfloat16),
            jax.ShapeDtypeStruct((n_blocks,) + labels.shape, jnp.int32),
        ],
        scratch_shapes=[
            pltpu.VMEM((w_rows, vp), jnp.bfloat16),
            pltpu.VMEM((rows, hid), jnp.bfloat16),
            pltpu.VMEM(labels.shape, jnp.int32),
            dma((3,)),
        ] + [dma((4,))] * 8 + [dma((8,))] * 2 + [dma((16,))] * 2,
        compiler_params=pltpu.CompilerParams(collective_id=0, has_side_effects=True, vmem_limit_bytes=VMEM_LIMIT),
        name="gather",
    )(w_pad, hidden, labels)


def _stats_kernel(st_ref, o_ref, got, s1, r1, s2, r2):
    n, n_z = 16, 4
    dp, zi, tp = lax.axis_index("dp"), lax.axis_index("fsdp"), lax.axis_index("tp")
    me = tp * n_z + zi

    def dev(p):
        return (dp, lax.rem(p, n_z), lax.div(p, n_z))

    peers = [lax.rem(me + o, n) for o in range(n)]
    barrier = pltpu.get_barrier_semaphore()
    for o in range(1, n):
        pl.semaphore_signal(barrier, inc=1, device_id=dev(peers[o]), device_id_type=MESH)
    pl.semaphore_wait(barrier, n - 1)
    first = [
        pltpu.make_async_remote_copy(st_ref.at[peers[o]], got.at[o], s1.at[o], r1.at[o], device_id=dev(peers[o]), device_id_type=MESH)
        for o in range(1, n)
    ]
    for copy in first:
        copy.start()
    got[0] = st_ref[me]
    for copy in first:
        copy.wait_recv()
    parts = [got[o] for o in range(n)]
    m_row = parts[0][0:1]
    for p in parts[1:]:
        m_row = jnp.maximum(m_row, p[0:1])
    s_row = jnp.zeros_like(m_row)
    t_row = jnp.zeros_like(m_row)
    for p in parts:
        s_row = s_row + p[1:2] * jnp.exp(p[0:1] - m_row)
        t_row = t_row + p[2:3]
    loss = m_row + jnp.log(s_row) - t_row
    o_ref[me] = jnp.concatenate([m_row, 1.0 / s_row, loss, m_row], axis=0)
    second = [
        pltpu.make_async_remote_copy(o_ref.at[me], o_ref.at[me], s2.at[o], r2.at[o], device_id=dev(peers[o]), device_id_type=MESH)
        for o in range(1, n)
    ]
    for copy in first:
        copy.wait_send()
    for copy in second:
        copy.start()
    for copy in second:
        copy.wait()


def _stats_call(st):
    n = st.shape[0]
    vmem = pl.BlockSpec(memory_space=pltpu.VMEM)
    return pl.pallas_call(
        _stats_kernel,
        in_specs=[vmem],
        out_specs=vmem,
        out_shape=jax.ShapeDtypeStruct(st.shape, jnp.float32),
        scratch_shapes=[pltpu.VMEM(st.shape, jnp.float32)] + [pltpu.SemaphoreType.DMA((n,))] * 4,
        compiler_params=pltpu.CompilerParams(collective_id=1, has_side_effects=True),
        name="stats",
    )(st)


def _logits_call(x_all, w, lab, valid):
    n_blocks, rows, hid = x_all.shape
    vp = w.shape[1]
    tokens = n_blocks * rows
    return pl.pallas_call(
        functools.partial(_logits_kernel, vp),
        grid=(n_blocks,),
        in_specs=[
            pl.BlockSpec(memory_space=pltpu.SMEM),
            pl.BlockSpec((1, rows, hid), lambda i: (i, 0, 0)),
            pl.BlockSpec((hid, vp), lambda i: (0, 0)),
            pl.BlockSpec((1, 8, rows), lambda i: (i, 0, 0)),
        ],
        out_specs=[
            pl.BlockSpec((1, rows, vp), lambda i: (i, 0, 0)),
            pl.BlockSpec((1, STATS, rows), lambda i: (i, 0, 0)),
            pl.BlockSpec((hid, rows), lambda i: (0, i)),
        ],
        out_shape=[
            jax.ShapeDtypeStruct((n_blocks, rows, vp), jnp.float32),
            jax.ShapeDtypeStruct((n_blocks, STATS, rows), jnp.float32),
            jax.ShapeDtypeStruct((hid, tokens), jnp.bfloat16),
        ],
        scratch_shapes=[pltpu.VMEM((rows, LANES), jnp.float32)] * 3 + [pltpu.VMEM((rows, LANES), jnp.int32)],
        compiler_params=pltpu.CompilerParams(vmem_limit_bytes=VMEM_LIMIT),
        cost_estimate=pl.CostEstimate(flops=2 * tokens * hid * vp, bytes_accessed=tokens * vp * 4, transcendentals=tokens * vp),
        name="logits_stats",
    )(valid, x_all, w, lab)


def _grad_call(c, ids, z, w, st, lab, g_all, v0, sub):
    n_blocks, rows, vp = z.shape
    hid = w.shape[0]
    nb = 4
    tokens = n_blocks * rows
    extra = [] if g_all is None else list(g_all)

    def tp_of(i, ids):
        core = lax.rem(ids[0] + 1 + lax.div(i, 2), 2)
        y = lax.rem(ids[1] + lax.rem(i, 2), 2)
        return y * 2 + core

    def at(i, ids):
        return (tp_of(i, ids), c, 0)

    def at_row(i, ids):
        return (tp_of(i, ids), 0, c)

    return pl.pallas_call(
        functools.partial(_grad_kernel, v0, 1.0 / tokens),
        grid_spec=pltpu.PrefetchScalarGridSpec(
            num_scalar_prefetch=1,
            grid=(n_blocks // nb,),
            in_specs=[
                pl.BlockSpec((nb, sub, vp), at),
                pl.BlockSpec((hid, vp), lambda i, ids: (0, 0)),
                pl.BlockSpec((nb, STATS, sub), at_row),
                pl.BlockSpec((nb, 8, sub), at_row),
            ] + [pl.BlockSpec(memory_space=pl.ANY)] * len(extra),
            out_specs=[
                pl.BlockSpec((nb, sub, v0), at),
                pl.BlockSpec((nb, sub, vp - v0), at),
                pl.BlockSpec((1, nb, sub, hid), lambda i, ids: (lax.max(i - 2, 0), 0, 0, 0)),
                pl.BlockSpec((1, nb, sub, hid), lambda i, ids: (lax.min(i, 1), 0, 0, 0)),
            ],
        ),
        out_shape=[
            jax.ShapeDtypeStruct((n_blocks, rows, v0), jnp.bfloat16),
            jax.ShapeDtypeStruct((n_blocks, rows, vp - v0), jnp.bfloat16),
            jax.ShapeDtypeStruct((2, nb, sub, hid), jnp.float32),
            jax.ShapeDtypeStruct((2, nb, sub, hid), jnp.float32),
        ],
        input_output_aliases={5: 0, 6: 1} if extra else {},
        compiler_params=pltpu.CompilerParams(vmem_limit_bytes=VMEM_LIMIT),
        cost_estimate=pl.CostEstimate(flops=2 * n_blocks * sub * hid * vp, bytes_accessed=n_blocks * sub * vp * 6, transcendentals=n_blocks * sub * vp),
        name="grad_dx",
    )(ids, z, w, st, lab, *extra)


def _dw_call(xt, g):
    hid, tokens = xt.shape
    sub, width = g.shape[1:]
    kb = 1024
    steps = tokens // kb
    return pl.pallas_call(
        functools.partial(_dw_kernel, steps),
        grid=(steps,),
        in_specs=[
            pl.BlockSpec((hid, kb), lambda k: (0, k)),
            pl.BlockSpec((kb // sub, sub, width), lambda k: (k, 0, 0)),
        ],
        out_specs=pl.BlockSpec((hid, width), lambda k: (0, 0)),
        out_shape=jax.ShapeDtypeStruct((hid, width), jnp.bfloat16),
        scratch_shapes=[pltpu.VMEM((hid, width), jnp.float32)],
        compiler_params=pltpu.CompilerParams(vmem_limit_bytes=VMEM_LIMIT),
        cost_estimate=pl.CostEstimate(flops=2 * tokens * hid * width, bytes_accessed=tokens * (width + hid) * 2, transcendentals=0),
        name="dw",
    )(xt, g)


def _place_kernel(n_z, v0, zi_ref, *refs):
    o_ref = refs[-1]
    j = pl.program_id(0)
    dist = lax.rem(zi_ref[0] + n_z - j, n_z)
    for s in range(n_z):
        @pl.when(dist == s)
        def _():
            o_ref[:, :v0] = refs[2 * s][...]
            o_ref[:, v0:] = refs[2 * s + 1][...]


def _place_call(zi, pieces, vp, vocab_dev):
    n_z = len(pieces) // 2
    rows, v0 = pieces[0].shape
    return pl.pallas_call(
        functools.partial(_place_kernel, n_z, v0),
        grid=(n_z,),
        in_specs=[pl.BlockSpec(memory_space=pltpu.SMEM)]
        + [pl.BlockSpec(p.shape, lambda j: (0, 0)) for p in pieces],
        out_specs=pl.BlockSpec((rows, vp), lambda j: (0, j)),
        out_shape=jax.ShapeDtypeStruct((rows, vocab_dev), jnp.bfloat16),
        compiler_params=pltpu.CompilerParams(vmem_limit_bytes=VMEM_LIMIT),
        name="place",
    )(zi, *pieces)


def _after(value, *deps):
    return lax.optimization_barrier((value,) + deps)[0]


def solution(mesh):
    n_z = mesh.shape["fsdp"]
    n_tp = mesh.shape["tp"]
    n_blocks = n_z * n_tp
    token_spec = P(("dp", "fsdp", "tp"), None)
    label_spec = P(("dp", "fsdp", "tp"))

    def z_shift(a, s):
        return lax.ppermute(a, "fsdp", [(k, (k + s) % n_z) for k in range(n_z)])

    def swap(a, axis, bit):
        return lax.ppermute(a, axis, [(k, k ^ bit) for k in range(mesh.shape[axis])])

    def pick(a, i, axis=0):
        return lax.dynamic_index_in_dim(a, i, axis, keepdims=False)

    def step(hidden, w_head, labels):
        rows_dev, hid = hidden.shape
        w_rows, vocab_dev = w_head.shape
        tokens = rows_dev * n_blocks
        vp = _ceil_to(-(-vocab_dev // n_z), LANES)
        sub = rows_dev // CHUNKS
        zi = lax.axis_index("fsdp")
        tpi = lax.axis_index("tp")
        yi, ci = tpi // 2, tpi % 2

        w_pad = jnp.pad(w_head, ((0, 0), (0, n_z * vp - vocab_dev)))
        w_full, x_all, lab = _gather_call(w_pad, hidden, labels.reshape(1, rows_dev), vp, n_blocks)

        lab = lab - (tpi * vocab_dev + zi * vp)
        valid = jnp.minimum(vocab_dev - zi * vp, vp).astype(jnp.int32)
        lab = jnp.where((lab >= 0) & (lab < valid), lab, -1 - 2 * LANES).astype(jnp.float32)
        lab = jnp.broadcast_to(lab, (n_blocks, 8, rows_dev))

        z_all, local, xt = _logits_call(x_all, w_full, lab, valid.reshape(1))
        st = _stats_call(local)
        mean_loss = (jnp.sum(st[:, 2]) * (1.0 / tokens)).reshape(1)

        v0 = _tiles(vp)[2][0]
        ids = jnp.stack([ci, yi]).astype(jnp.int32)

        def grad(c, g_all, *deps):
            i = _after(ids, *deps) if deps else ids
            g0, g1, keep, send = _grad_call(c, i, z_all, w_full, st, lab, g_all, v0, sub)
            return (g0, g1), keep, swap(send, "tp", 1)

        def to_y(c, *deps):
            keep = _after(keeps[c], *deps)
            other = keep[1] + gots[c][1]
            mine = keep[0] + gots[c][0]
            ys[c] = (mine, swap(other, "tp", 2))
            return mine, other

        def to_near(c, *deps):
            both = (_after(ys[c][0], *deps) + ys[c][1]).reshape(2, 2, sub, hid)
            odd = zi % 2
            mine, other = pick(both, odd, 1), pick(both, 1 - odd, 1)
            nears[c] = (mine, swap(other, "fsdp", 1))
            return mine, other

        def to_far(c, *deps):
            both = _after(nears[c][0], *deps) + nears[c][1]
            high = zi // 2
            mine, other = pick(both, high), pick(both, 1 - high)
            fars[c] = (mine, swap(other, "fsdp", 2))
            return mine, other

        def last(c, *deps):
            return (_after(fars[c][0], *deps) + fars[c][1]).astype(jnp.bfloat16)

        def send_dw(dw):
            parts = [pick(dw, (zi + s) % n_z) for s in range(n_z)]
            sent = [parts[0]]
            for s in range(1, n_z):
                sent.append(z_shift(parts[s], s))
            return parts, sent

        keeps, gots, ys, nears, fars = ([None] * CHUNKS for _ in range(5))
        g, keeps[0], gots[0] = grad(0, None)
        g, keeps[1], gots[1] = grad(1, g, keeps[0])
        t = to_y(0, keeps[1])
        g, keeps[2], gots[2] = grad(2, g, *t)
        t = to_y(1, keeps[2])
        g, keeps[3], gots[3] = grad(3, g, *t)
        t = to_y(2, keeps[3]) + to_near(0, keeps[3])
        dw0 = _dw_call(_after(xt, *t), g[0]).reshape(n_z, w_rows, v0)
        parts0, pieces0 = send_dw(dw0)
        t = to_y(3, dw0) + to_near(1, dw0) + to_far(0, dw0) + tuple(parts0)
        dw1 = _dw_call(_after(xt, *t), g[1]).reshape(n_z, w_rows, vp - v0)
        parts1, pieces1 = send_dw(dw1)
        t = to_near(2, *parts1)
        t = to_far(1, *t)
        t = to_near(3, *t)
        t = to_far(2, *t)
        t = to_far(3, *t)
        out = [last(c, *t) for c in range(CHUNKS)]
        pieces = [p for pair in zip(pieces0, pieces1) for p in pair]
        zv = _after(zi.reshape(1).astype(jnp.int32), *out)
        d_w = _place_call(zv, pieces, vp, vocab_dev)
        return mean_loss, jnp.concatenate(out, axis=0), d_w

    return jax.shard_map(
        step,
        mesh=mesh,
        in_specs=(token_spec, P("fsdp", "tp"), label_spec),
        out_specs=(P("dp"), token_spec, P(("dp", "fsdp"), "tp")),
        check_vma=False,
    )
```

```python
import functools

import jax
import jax.numpy as jnp
from jax import lax
from jax.experimental import pallas as pl
from jax.experimental.pallas import tpu as pltpu
from jax.sharding import PartitionSpec as P


LANES = 128
MESH = pl.DeviceIdType.MESH
NEG = -3.0e38
VMEM_LIMIT = 60 * 1024 * 1024
CHUNKS = 4
STATS = 4


def _ceil_to(n, m):
    return -(-n // m) * m


def _rows_to_cols(ref):
    cols = [jnp.concatenate([ref[b]] * (LANES // ref.shape[1]), axis=0).T for b in range(ref.shape[0])]
    return jnp.concatenate(cols, axis=0)


def _tiles(vp):
    width = vp // 4 // 256 * 256
    edges = [0, width, 2 * width, 3 * width, vp]
    return list(zip(edges[:-1], edges[1:]))


def _logits_block(x, w_ref, lab_row, valid, z_ref, xt_ref, m_ref, s_ref, t_ref, l_ref):
    rows = x.shape[0]
    vp = w_ref.shape[1]
    lane = lax.broadcasted_iota(jnp.int32, (rows, LANES), 1)
    lab = jnp.broadcast_to(lab_row.astype(jnp.float32), (LANES, rows)).T
    l_ref[...] = lab.astype(jnp.int32) - lane
    m_ref[...] = jnp.full((rows, LANES), NEG, jnp.float32)
    s_ref[...] = jnp.zeros((rows, LANES), jnp.float32)
    t_ref[...] = jnp.zeros((rows, LANES), jnp.float32)
    step = 32

    def stats(c0, c1):
        for r in range(0, rows, step):
            sl = slice(r, r + step)
            zs = [z_ref[sl, k:k + LANES] for k in range(c0, c1, LANES)]
            off = l_ref[sl, :]
            t = t_ref[sl, :]
            m_old = m_ref[sl, :]
            m = m_old
            for zk, k in zip(zs, range(c0, c1, LANES)):
                t = t + jnp.where(off == k, zk, 0.0)
                m = jnp.maximum(m, zk)
            s = s_ref[sl, :] * jnp.exp(m_old - m)
            for zk in zs:
                s = s + jnp.exp(zk - m)
            m_ref[sl, :] = m
            s_ref[sl, :] = s
            t_ref[sl, :] = t

    before = None
    for c0, c1 in _tiles(vp):
        z = jnp.dot(x, w_ref[:, c0:c1], preferred_element_type=jnp.float32)
        if c1 == vp:
            edge = (vp - 2 * LANES - c0) // LANES * LANES
            z_ref[:, c0:c0 + edge] = z[:, :edge]
            for k in range(edge, c1 - c0, LANES):
                z_ref[:, c0 + k:c0 + k + LANES] = jnp.where(lane < valid - (c0 + k), z[:, k:k + LANES], NEG)
        else:
            z_ref[:, c0:c1] = z
        if before is not None:
            stats(*before)
        before = (c0, c1)
    xt_ref[...] = x.T
    stats(*before)
    m = m_ref[...]
    m_row = jnp.max(m, axis=1, keepdims=True)
    s_row = jnp.sum(s_ref[...] * jnp.exp(m - m_row), axis=1, keepdims=True)
    t_row = jnp.sum(t_ref[...], axis=1, keepdims=True)
    packed = jnp.where(lane == 0, m_row, jnp.where(lane == 1, s_row, t_row))
    return packed.T[0:STATS, :]


def _grad_kernel(v0, inv_tokens, ids_ref, z_ref, w_ref, st_ref, lab_ref, *rest):
    g0_ref, g1_ref, keep_ref, send_ref = rest[-4:]
    blocks, sub, vp = z_ref.shape
    rows = blocks * sub
    st = _rows_to_cols(st_ref)
    m_row = st[:, 0:1]
    scale = st[:, 1:2] * inv_tokens
    lab_off = _rows_to_cols(lab_ref)[:, 0:1].astype(jnp.int32) - lax.broadcasted_iota(jnp.int32, (rows, LANES), 1)
    dims = (((1,), (1,)), ((), ()))

    for k in range(0, vp, LANES):
        p = jnp.exp(z_ref[:, :, k:k + LANES].reshape(rows, LANES) - m_row) * scale
        g = jnp.where(lab_off == k, p - inv_tokens, p).astype(jnp.bfloat16).reshape(blocks, sub, LANES)
        if k < v0:
            g0_ref[:, :, k:k + LANES] = g
        else:
            g1_ref[:, :, k - v0:k - v0 + LANES] = g
    total = lax.dot_general(g0_ref[...].reshape(rows, v0), w_ref[:, :v0], dims, preferred_element_type=jnp.float32)
    total = total + lax.dot_general(g1_ref[...].reshape(rows, vp - v0), w_ref[:, v0:], dims, preferred_element_type=jnp.float32)
    total = total.reshape(keep_ref.shape)
    i = pl.program_id(0)

    @pl.when(i < 2)
    def _():
        send_ref[...] = total

    @pl.when(i >= 2)
    def _():
        keep_ref[...] = total


def _dw_kernel(steps, xt_ref, g_ref, o_ref, acc_ref):
    k = pl.program_id(0)

    @pl.when(k == 0)
    def _():
        acc_ref[...] = jnp.zeros_like(acc_ref)

    g = g_ref[...].reshape(xt_ref.shape[1], g_ref.shape[2])
    acc_ref[...] += jnp.dot(xt_ref[...], g, preferred_element_type=jnp.float32)

    @pl.when(k == steps - 1)
    def _():
        o_ref[...] = acc_ref[...].astype(o_ref.dtype)


def _front_kernel(vocab_dev, w_ref, x_ref, l_ref, wo_ref, lo_ref, zo_ref, xto_ref, st_ref,
                  wv, xv, lv, zb, xtb, ms, ss, ts, ls, loc, z_sem, xt_sem,
                  w_s, w_r, wx_s, wx_r, x_s, x_r, y_s, y_r, c_s, c_r, l_s, l_r):
    n_z, n_tp = 4, 4
    n = n_z * n_tp
    dp, zi, tp = lax.axis_index("dp"), lax.axis_index("fsdp"), lax.axis_index("tp")
    w_rows = w_ref.shape[0]
    half = w_rows // 2
    vp = wv.shape[1]
    rows = x_ref.shape[0]
    mine = tp * n_z + zi

    def dev(p):
        return (dp, lax.rem(p, n_z), lax.div(p, n_z))

    def flip(v, j):
        high = lax.rem(lax.div(v, 2) + j // 2, 2)
        low = lax.rem(lax.rem(v, 2) + lax.rem(j, 2), 2)
        return high * 2 + low

    peers = [dev(lax.rem(mine + o, n)) for o in range(n)]
    y_tp, c_tp = flip(tp, 2), flip(tp, 1)
    y_dev, c_dev, x_dev = (dp, zi, y_tp), (dp, zi, c_tp), (1 - dp, zi, tp)
    z_owner = [flip(zi, j) for j in range(n_z)]
    near_dev, far_dev = (dp, z_owner[1], tp), (dp, z_owner[2], tp)

    barrier = pltpu.get_barrier_semaphore()
    for d in peers[1:] + [x_dev]:
        pl.semaphore_signal(barrier, inc=1, device_id=d, device_id_type=MESH)
    pl.semaphore_wait(barrier, n)

    def remote(src, dst, s_sem, r_sem, d):
        return pltpu.make_async_remote_copy(src, dst, s_sem, r_sem, device_id=d, device_id_type=MESH)

    def w_half(owner, part):
        return wv.at[pl.ds(pl.multiple_of(owner * w_rows + part * half, 8), half), :]

    def w_cols(z):
        return pl.ds(pl.multiple_of(z * vp, LANES), vp)

    load_x = pltpu.make_async_copy(x_ref, xv.at[mine], loc.at[0])
    load_w = pltpu.make_async_copy(w_ref.at[:, w_cols(zi)], wv.at[pl.ds(pl.multiple_of(zi * w_rows, 8), w_rows), :], loc.at[1])
    load_l = pltpu.make_async_copy(l_ref, lv.at[mine], loc.at[2])
    load_x.start()
    load_w.start()
    load_l.start()
    l_in = [remote(l_ref, lv.at[mine], l_s.at[o], l_r.at[o], peers[o]) for o in range(1, n)]
    w_in = [None] + [
        remote(w_ref.at[pl.ds(pl.multiple_of(dp * half, 8), half), w_cols(z_owner[k])], w_half(zi, dp),
               w_s.at[k], w_r.at[k], (dp, z_owner[k], tp))
        for k in range(1, n_z)
    ]

    def own(j):
        return xv.at[tp * n_z + z_owner[j]]

    def partner(j):
        return xv.at[y_tp * n_z + z_owner[j]]

    x_in = [None, remote(x_ref, xv.at[mine], x_s.at[1], x_r.at[1], near_dev),
            remote(x_ref, xv.at[mine], x_s.at[2], x_r.at[2], far_dev),
            remote(own(2), own(2), x_s.at[3], x_r.at[3], near_dev)]
    y_in = [remote(own(j) if j else x_ref, own(j), y_s.at[j], y_r.at[j], y_dev) for j in range(n_z)]
    c_in = [remote(own(j) if j else x_ref, own(j), c_s.at[j], c_r.at[j], c_dev) for j in range(n_z)]
    c_in += [remote(partner(j), partner(j), c_s.at[n_z + j], c_r.at[n_z + j], c_dev) for j in range(n_z)]
    wx_in = [None] + [
        remote(w_half(z_owner[k], dp), w_half(z_owner[k], dp), wx_s.at[k], wx_r.at[k], x_dev)
        for k in range(1, n_z)
    ]

    def from_x(j):
        x_in[j].wait_recv()
        if j == 2:
            x_in[3].start()
        y_in[j].start()
        c_in[j].start()

    def from_y(j):
        y_in[j].wait_recv()
        c_in[n_z + j].start()

    def from_w(k):
        w_in[k].wait_recv()
        wx_in[k].start()

    for copy in [y_in[0], c_in[0]] + l_in + [w_in[1], x_in[1], w_in[2], w_in[3], x_in[2]]:
        copy.start()
    from_w(1)
    from_y(0)
    from_x(1)
    from_w(2)
    from_y(1)
    from_w(3)
    for copy in l_in:
        copy.wait_recv()
    for copy in (load_x, load_w, load_l):
        copy.wait()
    save_l = pltpu.make_async_copy(lv, lo_ref, loc.at[2])
    save_l.start()
    for copy in wx_in[1:]:
        copy.wait_recv()
    save_w = pltpu.make_async_copy(wv, wo_ref, loc.at[1])
    save_w.start()

    before = {2: [lambda: from_x(2)], 7: [lambda: from_y(2)], 8: [lambda: from_x(3)], 11: [lambda: from_y(3)]}
    for j in range(n_z):
        before.setdefault(4 * j + 1, []).append(c_in[j].wait_recv)
        before.setdefault(4 * j + 3, []).append(c_in[n_z + j].wait_recv)

    first_col = tp * vocab_dev + zi * vp
    valid = lax.min(vocab_dev - zi * vp, vp)

    def outs(slot, block):
        return (pltpu.make_async_copy(zb.at[slot], zo_ref.at[block], z_sem.at[slot]),
                pltpu.make_async_copy(xtb.at[slot], xto_ref.at[:, pl.ds(pl.multiple_of(block * rows, LANES), rows)], xt_sem.at[slot]))

    def body(it, carry):
        owner = flip(zi, it // 2)
        for slot in range(2):
            for i in range(slot, n, 2):
                if i in before:
                    @pl.when(it == i // 2)
                    def _():
                        for act in before[i]:
                            act()
            block = flip(tp, lax.rem(it, 2) * 2 + slot) * n_z + owner

            @pl.when(it > 0)
            def _():
                for copy in outs(slot, block):
                    copy.wait()

            lab = lv[block] - first_col
            lab = jnp.where((lab >= 0) & (lab < valid), lab, -1 - 2 * LANES)
            st_ref[block] = _logits_block(xv[block], wv, lab, valid, zb.at[slot], xtb.at[slot],
                                          ms.at[slot], ss.at[slot], ts.at[slot], ls.at[slot])
            for copy in outs(slot, block):
                copy.start()
        return carry

    lax.fori_loop(0, n // 2, body, 0)
    for slot in range(2):
        for copy in outs(slot, mine):
            copy.wait()
    for copy in l_in + w_in[1:] + x_in[1:] + y_in + c_in + wx_in[1:]:
        copy.wait_send()
    save_w.wait()
    save_l.wait()


def _front_call(w_pad, hidden, labels, vp, vocab_dev, n_blocks):
    rows, hid = hidden.shape
    tokens = n_blocks * rows
    dma = pltpu.SemaphoreType.DMA
    hbm = pl.BlockSpec(memory_space=pl.ANY)
    return pl.pallas_call(
        functools.partial(_front_kernel, vocab_dev),
        in_specs=[hbm] * 3,
        out_specs=[hbm] * 4 + [pl.BlockSpec(memory_space=pltpu.VMEM)],
        out_shape=[
            jax.ShapeDtypeStruct((hid, vp), jnp.bfloat16),
            jax.ShapeDtypeStruct((n_blocks,) + labels.shape, jnp.int32),
            jax.ShapeDtypeStruct((n_blocks, rows, vp), jnp.float32),
            jax.ShapeDtypeStruct((hid, tokens), jnp.bfloat16),
            jax.ShapeDtypeStruct((n_blocks, STATS, rows), jnp.float32),
        ],
        scratch_shapes=[
            pltpu.VMEM((hid, vp), jnp.bfloat16),
            pltpu.VMEM((n_blocks, rows, hid), jnp.bfloat16),
            pltpu.VMEM((n_blocks,) + labels.shape, jnp.int32),
            pltpu.VMEM((2, rows, vp), jnp.float32),
            pltpu.VMEM((2, hid, rows), jnp.bfloat16),
        ] + [pltpu.VMEM((2, rows, LANES), jnp.float32)] * 3 + [
            pltpu.VMEM((2, rows, LANES), jnp.int32),
            dma((3,)), dma((2,)), dma((2,)),
        ] + [dma((4,))] * 8 + [dma((8,))] * 2 + [dma((16,))] * 2,
        compiler_params=pltpu.CompilerParams(collective_id=0, has_side_effects=True, vmem_limit_bytes=VMEM_LIMIT),
        name="front",
    )(w_pad, hidden, labels)


def _stats_kernel(st_ref, o_ref, got, s1, r1, s2, r2):
    n, n_z = 16, 4
    dp, zi, tp = lax.axis_index("dp"), lax.axis_index("fsdp"), lax.axis_index("tp")
    me = tp * n_z + zi

    def dev(p):
        return (dp, lax.rem(p, n_z), lax.div(p, n_z))

    peers = [lax.rem(me + o, n) for o in range(n)]
    barrier = pltpu.get_barrier_semaphore()
    for o in range(1, n):
        pl.semaphore_signal(barrier, inc=1, device_id=dev(peers[o]), device_id_type=MESH)
    pl.semaphore_wait(barrier, n - 1)
    first = [
        pltpu.make_async_remote_copy(st_ref.at[peers[o]], got.at[o], s1.at[o], r1.at[o], device_id=dev(peers[o]), device_id_type=MESH)
        for o in range(1, n)
    ]
    for copy in first:
        copy.start()
    got[0] = st_ref[me]
    for copy in first:
        copy.wait_recv()
    parts = [got[o] for o in range(n)]
    m_row = parts[0][0:1]
    for p in parts[1:]:
        m_row = jnp.maximum(m_row, p[0:1])
    s_row = jnp.zeros_like(m_row)
    t_row = jnp.zeros_like(m_row)
    for p in parts:
        s_row = s_row + p[1:2] * jnp.exp(p[0:1] - m_row)
        t_row = t_row + p[2:3]
    loss = m_row + jnp.log(s_row) - t_row
    o_ref[me] = jnp.concatenate([m_row, 1.0 / s_row, loss, m_row], axis=0)
    second = [
        pltpu.make_async_remote_copy(o_ref.at[me], o_ref.at[me], s2.at[o], r2.at[o], device_id=dev(peers[o]), device_id_type=MESH)
        for o in range(1, n)
    ]
    for copy in first:
        copy.wait_send()
    for copy in second:
        copy.start()
    for copy in second:
        copy.wait()


def _stats_call(st):
    n = st.shape[0]
    vmem = pl.BlockSpec(memory_space=pltpu.VMEM)
    return pl.pallas_call(
        _stats_kernel,
        in_specs=[vmem],
        out_specs=vmem,
        out_shape=jax.ShapeDtypeStruct(st.shape, jnp.float32),
        scratch_shapes=[pltpu.VMEM(st.shape, jnp.float32)] + [pltpu.SemaphoreType.DMA((n,))] * 4,
        compiler_params=pltpu.CompilerParams(collective_id=1, has_side_effects=True),
        name="stats",
    )(st)


def _grad_call(c, ids, z, w, st, lab, g_all, v0, sub):
    n_blocks, rows, vp = z.shape
    hid = w.shape[0]
    nb = 4
    tokens = n_blocks * rows
    extra = [] if g_all is None else list(g_all)

    def tp_of(i, ids):
        core = lax.rem(ids[0] + 1 + lax.div(i, 2), 2)
        y = lax.rem(ids[1] + lax.rem(i, 2), 2)
        return y * 2 + core

    def at(i, ids):
        return (tp_of(i, ids), c, 0)

    def at_row(i, ids):
        return (tp_of(i, ids), 0, c)

    return pl.pallas_call(
        functools.partial(_grad_kernel, v0, 1.0 / tokens),
        grid_spec=pltpu.PrefetchScalarGridSpec(
            num_scalar_prefetch=1,
            grid=(n_blocks // nb,),
            in_specs=[
                pl.BlockSpec((nb, sub, vp), at),
                pl.BlockSpec((hid, vp), lambda i, ids: (0, 0)),
                pl.BlockSpec((nb, STATS, sub), at_row),
                pl.BlockSpec((nb, 8, sub), at_row),
            ] + [pl.BlockSpec(memory_space=pl.ANY)] * len(extra),
            out_specs=[
                pl.BlockSpec((nb, sub, v0), at),
                pl.BlockSpec((nb, sub, vp - v0), at),
                pl.BlockSpec((1, nb, sub, hid), lambda i, ids: (lax.max(i - 2, 0), 0, 0, 0)),
                pl.BlockSpec((1, nb, sub, hid), lambda i, ids: (lax.min(i, 1), 0, 0, 0)),
            ],
        ),
        out_shape=[
            jax.ShapeDtypeStruct((n_blocks, rows, v0), jnp.bfloat16),
            jax.ShapeDtypeStruct((n_blocks, rows, vp - v0), jnp.bfloat16),
            jax.ShapeDtypeStruct((2, nb, sub, hid), jnp.float32),
            jax.ShapeDtypeStruct((2, nb, sub, hid), jnp.float32),
        ],
        input_output_aliases={5: 0, 6: 1} if extra else {},
        compiler_params=pltpu.CompilerParams(vmem_limit_bytes=VMEM_LIMIT),
        cost_estimate=pl.CostEstimate(flops=2 * n_blocks * sub * hid * vp, bytes_accessed=n_blocks * sub * vp * 6, transcendentals=n_blocks * sub * vp),
        name="grad_dx",
    )(ids, z, w, st, lab, *extra)


def _dw_call(xt, g):
    hid, tokens = xt.shape
    sub, width = g.shape[1:]
    kb = 1024
    steps = tokens // kb
    return pl.pallas_call(
        functools.partial(_dw_kernel, steps),
        grid=(steps,),
        in_specs=[
            pl.BlockSpec((hid, kb), lambda k: (0, k)),
            pl.BlockSpec((kb // sub, sub, width), lambda k: (k, 0, 0)),
        ],
        out_specs=pl.BlockSpec((hid, width), lambda k: (0, 0)),
        out_shape=jax.ShapeDtypeStruct((hid, width), jnp.bfloat16),
        scratch_shapes=[pltpu.VMEM((hid, width), jnp.float32)],
        compiler_params=pltpu.CompilerParams(vmem_limit_bytes=VMEM_LIMIT),
        cost_estimate=pl.CostEstimate(flops=2 * tokens * hid * width, bytes_accessed=tokens * (width + hid) * 2, transcendentals=0),
        name="dw",
    )(xt, g)


def _place_kernel(n_z, v0, zi_ref, *refs):
    o_ref = refs[-1]
    j = pl.program_id(0)
    dist = lax.rem(zi_ref[0] + n_z - j, n_z)
    for s in range(n_z):
        @pl.when(dist == s)
        def _():
            o_ref[:, :v0] = refs[2 * s][...]
            o_ref[:, v0:] = refs[2 * s + 1][...]


def _place_call(zi, pieces, vp, vocab_dev):
    n_z = len(pieces) // 2
    rows, v0 = pieces[0].shape
    return pl.pallas_call(
        functools.partial(_place_kernel, n_z, v0),
        grid=(n_z,),
        in_specs=[pl.BlockSpec(memory_space=pltpu.SMEM)]
        + [pl.BlockSpec(p.shape, lambda j: (0, 0)) for p in pieces],
        out_specs=pl.BlockSpec((rows, vp), lambda j: (0, j)),
        out_shape=jax.ShapeDtypeStruct((rows, vocab_dev), jnp.bfloat16),
        compiler_params=pltpu.CompilerParams(vmem_limit_bytes=VMEM_LIMIT),
        name="place",
    )(zi, *pieces)


def _after(value, *deps):
    return lax.optimization_barrier((value,) + deps)[0]


def solution(mesh):
    n_z = mesh.shape["fsdp"]
    n_tp = mesh.shape["tp"]
    n_blocks = n_z * n_tp
    token_spec = P(("dp", "fsdp", "tp"), None)
    label_spec = P(("dp", "fsdp", "tp"))

    def z_shift(a, s):
        return lax.ppermute(a, "fsdp", [(k, (k + s) % n_z) for k in range(n_z)])

    def swap(a, axis, bit):
        return lax.ppermute(a, axis, [(k, k ^ bit) for k in range(mesh.shape[axis])])

    def pick(a, i, axis=0):
        return lax.dynamic_index_in_dim(a, i, axis, keepdims=False)

    def step(hidden, w_head, labels):
        rows_dev, hid = hidden.shape
        w_rows, vocab_dev = w_head.shape
        tokens = rows_dev * n_blocks
        vp = _ceil_to(-(-vocab_dev // n_z), LANES)
        sub = rows_dev // CHUNKS
        zi = lax.axis_index("fsdp")
        tpi = lax.axis_index("tp")
        yi, ci = tpi // 2, tpi % 2

        w_pad = jnp.pad(w_head, ((0, 0), (0, n_z * vp - vocab_dev)))
        w_full, lab, z_all, xt, local = _front_call(w_pad, hidden, labels.reshape(1, rows_dev), vp, vocab_dev, n_blocks)

        lab = lab - (tpi * vocab_dev + zi * vp)
        valid = jnp.minimum(vocab_dev - zi * vp, vp).astype(jnp.int32)
        lab = jnp.where((lab >= 0) & (lab < valid), lab, -1 - 2 * LANES).astype(jnp.float32)
        lab = jnp.broadcast_to(lab, (n_blocks, 8, rows_dev))

        st = _stats_call(local)
        mean_loss = (jnp.sum(st[:, 2]) * (1.0 / tokens)).reshape(1)

        v0 = _tiles(vp)[2][0]
        ids = jnp.stack([ci, yi]).astype(jnp.int32)

        def grad(c, g_all, *deps):
            i = _after(ids, *deps) if deps else ids
            g0, g1, keep, send = _grad_call(c, i, z_all, w_full, st, lab, g_all, v0, sub)
            return (g0, g1), keep, swap(send, "tp", 1)

        def to_y(c, *deps):
            keep = _after(keeps[c], *deps)
            other = keep[1] + gots[c][1]
            mine = keep[0] + gots[c][0]
            ys[c] = (mine, swap(other, "tp", 2))
            return mine, other

        def to_near(c, *deps):
            both = (_after(ys[c][0], *deps) + ys[c][1]).reshape(2, 2, sub, hid)
            odd = zi % 2
            mine, other = pick(both, odd, 1), pick(both, 1 - odd, 1)
            nears[c] = (mine, swap(other, "fsdp", 1))
            return mine, other

        def to_far(c, *deps):
            both = _after(nears[c][0], *deps) + nears[c][1]
            high = zi // 2
            mine, other = pick(both, high), pick(both, 1 - high)
            fars[c] = (mine, swap(other, "fsdp", 2))
            return mine, other

        def last(c, *deps):
            return (_after(fars[c][0], *deps) + fars[c][1]).astype(jnp.bfloat16)

        def send_dw(dw):
            parts = [pick(dw, (zi + s) % n_z) for s in range(n_z)]
            sent = [parts[0]]
            for s in range(1, n_z):
                sent.append(z_shift(parts[s], s))
            return parts, sent

        def wide_near(c, *deps):
            both = (_after(keeps[c], *deps) + gots[c]).reshape(2, 2, 2, sub, hid)
            odd = zi % 2
            mine, other = pick(both, odd, 2), pick(both, 1 - odd, 2)
            nears[c] = (mine, swap(other, "fsdp", 1))
            return mine, other

        def wide_far(c, *deps):
            both = _after(nears[c][0], *deps) + nears[c][1]
            high = zi // 2
            mine, other = pick(both, high, 1), pick(both, 1 - high, 1)
            fars[c] = (mine, swap(other, "fsdp", 2))
            return mine, other

        def wide_y(c, *deps):
            both = _after(fars[c][0], *deps) + fars[c][1]
            fars[c] = (both[0], swap(both[1], "tp", 2))
            return (both,)

        keeps, gots, ys, nears, fars = ([None] * CHUNKS for _ in range(5))
        g, keeps[0], gots[0] = grad(0, None)
        g, keeps[1], gots[1] = grad(1, g, keeps[0])
        t = wide_near(0, keeps[1])
        g, keeps[2], gots[2] = grad(2, g, *t)
        t = to_y(1, keeps[2])
        g, keeps[3], gots[3] = grad(3, g, *t)
        t = to_y(2, keeps[3]) + wide_far(0, keeps[3])
        dw0 = _dw_call(_after(xt, *t), g[0]).reshape(n_z, w_rows, v0)
        parts0, pieces0 = send_dw(dw0)
        t = to_near(1, dw0) + to_y(3, dw0) + wide_y(0, dw0) + tuple(parts0)
        dw1 = _dw_call(_after(xt, *t), g[1]).reshape(n_z, w_rows, vp - v0)
        parts1, pieces1 = send_dw(dw1)
        t = to_near(2, *parts1)
        t = to_far(1, *t)
        t = to_near(3, *t)
        t = to_far(2, *t)
        t = to_far(3, *t)
        out = [last(c, *t) for c in range(CHUNKS)]
        pieces = [p for pair in zip(pieces0, pieces1) for p in pair]
        zv = _after(zi.reshape(1).astype(jnp.int32), *out)
        d_w = _place_call(zv, pieces, vp, vocab_dev)
        return mean_loss, jnp.concatenate(out, axis=0), d_w

    return jax.shard_map(
        step,
        mesh=mesh,
        in_specs=(token_spec, P("fsdp", "tp"), label_spec),
        out_specs=(P("dp"), token_spec, P(("dp", "fsdp"), "tp")),
        check_vma=False,
    )
```

```python
import functools

import jax
import jax.numpy as jnp
from jax import lax
from jax.experimental import pallas as pl
from jax.experimental.pallas import tpu as pltpu
from jax.sharding import PartitionSpec as P


LANES = 128
MESH = pl.DeviceIdType.MESH
NEG = -3.0e38
VMEM_LIMIT = 60 * 1024 * 1024
CHUNKS = 4
STATS = 4


def _ceil_to(n, m):
    return -(-n // m) * m


def _rows_to_cols(ref):
    cols = [jnp.concatenate([ref[b]] * (LANES // ref.shape[1]), axis=0).T for b in range(ref.shape[0])]
    return jnp.concatenate(cols, axis=0)


def _tiles(vp):
    width = vp // 4 // 256 * 256
    edges = [0, width, 2 * width, 3 * width, vp]
    return list(zip(edges[:-1], edges[1:]))


def _logits_block(x, w_ref, lab_row, valid, z_ref, xt_ref, m_ref, s_ref, t_ref, l_ref):
    rows = x.shape[0]
    vp = w_ref.shape[1]
    lane = lax.broadcasted_iota(jnp.int32, (rows, LANES), 1)
    lab = jnp.broadcast_to(lab_row.astype(jnp.float32), (LANES, rows)).T
    l_ref[...] = lab.astype(jnp.int32) - lane
    m_ref[...] = jnp.full((rows, LANES), NEG, jnp.float32)
    s_ref[...] = jnp.zeros((rows, LANES), jnp.float32)
    t_ref[...] = jnp.zeros((rows, LANES), jnp.float32)
    step = 32

    def stats(c0, c1):
        for r in range(0, rows, step):
            sl = slice(r, r + step)
            zs = [z_ref[sl, k:k + LANES] for k in range(c0, c1, LANES)]
            off = l_ref[sl, :]
            t = t_ref[sl, :]
            m_old = m_ref[sl, :]
            m = m_old
            for zk, k in zip(zs, range(c0, c1, LANES)):
                t = t + jnp.where(off == k, zk, 0.0)
                m = jnp.maximum(m, zk)
            s = s_ref[sl, :] * jnp.exp(m_old - m)
            for zk in zs:
                s = s + jnp.exp(zk - m)
            m_ref[sl, :] = m
            s_ref[sl, :] = s
            t_ref[sl, :] = t

    before = None
    for c0, c1 in _tiles(vp):
        z = jnp.dot(x, w_ref[:, c0:c1], preferred_element_type=jnp.float32)
        if c1 == vp:
            edge = (vp - 2 * LANES - c0) // LANES * LANES
            z_ref[:, c0:c0 + edge] = z[:, :edge]
            for k in range(edge, c1 - c0, LANES):
                z_ref[:, c0 + k:c0 + k + LANES] = jnp.where(lane < valid - (c0 + k), z[:, k:k + LANES], NEG)
        else:
            z_ref[:, c0:c1] = z
        if before is not None:
            stats(*before)
        before = (c0, c1)
    xt_ref[...] = x.T
    stats(*before)
    m = m_ref[...]
    m_row = jnp.max(m, axis=1, keepdims=True)
    s_row = jnp.sum(s_ref[...] * jnp.exp(m - m_row), axis=1, keepdims=True)
    t_row = jnp.sum(t_ref[...], axis=1, keepdims=True)
    packed = jnp.where(lane == 0, m_row, jnp.where(lane == 1, s_row, t_row))
    return packed.T[0:STATS, :]


def _grad_kernel(v0, inv_tokens, ids_ref, z_ref, w_ref, st_ref, lab_ref, *rest):
    g0_ref, g1_ref, keep_ref, send_ref = rest[-4:]
    blocks, sub, vp = z_ref.shape
    rows = blocks * sub
    st = _rows_to_cols(st_ref)
    m_row = st[:, 0:1]
    scale = st[:, 1:2] * inv_tokens
    lab_off = _rows_to_cols(lab_ref)[:, 0:1].astype(jnp.int32) - lax.broadcasted_iota(jnp.int32, (rows, LANES), 1)
    dims = (((1,), (1,)), ((), ()))

    for k in range(0, vp, LANES):
        p = jnp.exp(z_ref[:, :, k:k + LANES].reshape(rows, LANES) - m_row) * scale
        g = jnp.where(lab_off == k, p - inv_tokens, p).astype(jnp.bfloat16).reshape(blocks, sub, LANES)
        if k < v0:
            g0_ref[:, :, k:k + LANES] = g
        else:
            g1_ref[:, :, k - v0:k - v0 + LANES] = g
    total = lax.dot_general(g0_ref[...].reshape(rows, v0), w_ref[:, :v0], dims, preferred_element_type=jnp.float32)
    total = total + lax.dot_general(g1_ref[...].reshape(rows, vp - v0), w_ref[:, v0:], dims, preferred_element_type=jnp.float32)
    total = total.reshape(keep_ref.shape)
    i = pl.program_id(0)

    @pl.when(i < 2)
    def _():
        send_ref[...] = total

    @pl.when(i >= 2)
    def _():
        keep_ref[...] = total


def _dw_kernel(steps, xt_ref, g_ref, o_ref, acc_ref):
    k = pl.program_id(0)

    @pl.when(k == 0)
    def _():
        acc_ref[...] = jnp.zeros_like(acc_ref)

    g = g_ref[...].reshape(xt_ref.shape[1], g_ref.shape[2])
    acc_ref[...] += jnp.dot(xt_ref[...], g, preferred_element_type=jnp.float32)

    @pl.when(k == steps - 1)
    def _():
        o_ref[...] = acc_ref[...].astype(o_ref.dtype)


def _front_kernel(vocab_dev, w_ref, x_ref, l_ref, wo_ref, lo_ref, zo_ref, xto_ref, st_ref,
                  wv, xv, lv, zb, xtb, ms, ss, ts, ls, loc, z_sem, xt_sem,
                  w_s, w_r, wx_s, wx_r, x_s, x_r, y_s, y_r, c_s, c_r, l_s, l_r):
    n_z, n_tp = 4, 4
    n = n_z * n_tp
    dp, zi, tp = lax.axis_index("dp"), lax.axis_index("fsdp"), lax.axis_index("tp")
    w_rows = w_ref.shape[0]
    half = w_rows // 2
    vp = wv.shape[1]
    rows = x_ref.shape[0]
    mine = tp * n_z + zi

    def dev(p):
        return (dp, lax.rem(p, n_z), lax.div(p, n_z))

    def flip(v, j):
        high = lax.rem(lax.div(v, 2) + j // 2, 2)
        low = lax.rem(lax.rem(v, 2) + lax.rem(j, 2), 2)
        return high * 2 + low

    peers = [dev(lax.rem(mine + o, n)) for o in range(n)]
    y_tp, c_tp = flip(tp, 2), flip(tp, 1)
    y_dev, c_dev, x_dev = (dp, zi, y_tp), (dp, zi, c_tp), (1 - dp, zi, tp)
    z_owner = [flip(zi, j) for j in range(n_z)]
    near_dev, far_dev = (dp, z_owner[1], tp), (dp, z_owner[2], tp)

    barrier = pltpu.get_barrier_semaphore()
    for d in peers[1:] + [x_dev]:
        pl.semaphore_signal(barrier, inc=1, device_id=d, device_id_type=MESH)
    pl.semaphore_wait(barrier, n)

    def remote(src, dst, s_sem, r_sem, d):
        return pltpu.make_async_remote_copy(src, dst, s_sem, r_sem, device_id=d, device_id_type=MESH)

    def w_half(owner, part):
        return wv.at[pl.ds(pl.multiple_of(owner * w_rows + part * half, 8), half), :]

    def w_cols(z):
        return pl.ds(pl.multiple_of(z * vp, LANES), vp)

    load_x = pltpu.make_async_copy(x_ref, xv.at[mine], loc.at[0])
    load_w = pltpu.make_async_copy(w_ref.at[:, w_cols(zi)], wv.at[pl.ds(pl.multiple_of(zi * w_rows, 8), w_rows), :], loc.at[1])
    load_l = pltpu.make_async_copy(l_ref, lv.at[mine], loc.at[2])
    load_x.start()
    load_w.start()
    load_l.start()
    l_in = [remote(l_ref, lv.at[mine], l_s.at[o], l_r.at[o], peers[o]) for o in range(1, n)]
    w_in = [None] + [
        remote(w_ref.at[pl.ds(pl.multiple_of(dp * half, 8), half), w_cols(z_owner[k])], w_half(zi, dp),
               w_s.at[k], w_r.at[k], (dp, z_owner[k], tp))
        for k in range(1, n_z)
    ]

    def own(j):
        return xv.at[tp * n_z + z_owner[j]]

    def partner(j):
        return xv.at[y_tp * n_z + z_owner[j]]

    x_in = [None, remote(x_ref, xv.at[mine], x_s.at[1], x_r.at[1], near_dev),
            remote(x_ref, xv.at[mine], x_s.at[2], x_r.at[2], far_dev),
            remote(own(2), own(2), x_s.at[3], x_r.at[3], near_dev)]
    y_in = [remote(own(j) if j else x_ref, own(j), y_s.at[j], y_r.at[j], y_dev) for j in range(n_z)]
    c_in = [remote(own(j) if j else x_ref, own(j), c_s.at[j], c_r.at[j], c_dev) for j in range(n_z)]
    c_in += [remote(partner(j), partner(j), c_s.at[n_z + j], c_r.at[n_z + j], c_dev) for j in range(n_z)]
    wx_in = [None] + [
        remote(w_half(z_owner[k], dp), w_half(z_owner[k], dp), wx_s.at[k], wx_r.at[k], x_dev)
        for k in range(1, n_z)
    ]

    def from_x(j):
        x_in[j].wait_recv()
        if j == 2:
            x_in[3].start()
        y_in[j].start()
        c_in[j].start()

    def from_y(j):
        y_in[j].wait_recv()
        c_in[n_z + j].start()

    def from_w(k):
        w_in[k].wait_recv()
        wx_in[k].start()

    for copy in [y_in[0], c_in[0]] + l_in + [w_in[1], x_in[1], w_in[2], w_in[3], x_in[2]]:
        copy.start()
    from_w(1)
    from_y(0)
    from_x(1)
    from_w(2)
    from_y(1)
    from_w(3)
    for copy in l_in:
        copy.wait_recv()
    for copy in (load_x, load_w, load_l):
        copy.wait()
    save_l = pltpu.make_async_copy(lv, lo_ref, loc.at[2])
    save_l.start()
    for copy in wx_in[1:]:
        copy.wait_recv()
    save_w = pltpu.make_async_copy(wv, wo_ref, loc.at[1])
    save_w.start()

    before = {2: [lambda: from_x(2)], 7: [lambda: from_y(2)], 8: [lambda: from_x(3)], 11: [lambda: from_y(3)]}
    for j in range(n_z):
        before.setdefault(4 * j + 1, []).append(c_in[j].wait_recv)
        before.setdefault(4 * j + 3, []).append(c_in[n_z + j].wait_recv)

    first_col = tp * vocab_dev + zi * vp
    valid = lax.min(vocab_dev - zi * vp, vp)

    def outs(slot, block):
        return (pltpu.make_async_copy(zb.at[slot], zo_ref.at[block], z_sem.at[slot]),
                pltpu.make_async_copy(xtb.at[slot], xto_ref.at[:, pl.ds(pl.multiple_of(block * rows, LANES), rows)], xt_sem.at[slot]))

    def body(it, carry):
        owner = flip(zi, it // 2)
        for slot in range(2):
            for i in range(slot, n, 2):
                if i in before:
                    @pl.when(it == i // 2)
                    def _():
                        for act in before[i]:
                            act()
            block = flip(tp, lax.rem(it, 2) * 2 + slot) * n_z + owner

            @pl.when(it > 0)
            def _():
                for copy in outs(slot, block):
                    copy.wait()

            lab = lv[block] - first_col
            lab = jnp.where((lab >= 0) & (lab < valid), lab, -1 - 2 * LANES)
            st_ref[block] = _logits_block(xv[block], wv, lab, valid, zb.at[slot], xtb.at[slot],
                                          ms.at[slot], ss.at[slot], ts.at[slot], ls.at[slot])
            for copy in outs(slot, block):
                copy.start()
        return carry

    lax.fori_loop(0, n // 2, body, 0)
    for slot in range(2):
        for copy in outs(slot, mine):
            copy.wait()
    for copy in l_in + w_in[1:] + x_in[1:] + y_in + c_in + wx_in[1:]:
        copy.wait_send()
    save_w.wait()
    save_l.wait()


def _front_call(w_pad, hidden, labels, vp, vocab_dev, n_blocks):
    rows, hid = hidden.shape
    tokens = n_blocks * rows
    dma = pltpu.SemaphoreType.DMA
    hbm = pl.BlockSpec(memory_space=pl.ANY)
    return pl.pallas_call(
        functools.partial(_front_kernel, vocab_dev),
        in_specs=[hbm] * 3,
        out_specs=[hbm] * 4 + [pl.BlockSpec(memory_space=pltpu.VMEM)],
        out_shape=[
            jax.ShapeDtypeStruct((hid, vp), jnp.bfloat16),
            jax.ShapeDtypeStruct((n_blocks,) + labels.shape, jnp.int32),
            jax.ShapeDtypeStruct((n_blocks, rows, vp), jnp.float32),
            jax.ShapeDtypeStruct((hid, tokens), jnp.bfloat16),
            jax.ShapeDtypeStruct((n_blocks, STATS, rows), jnp.float32),
        ],
        scratch_shapes=[
            pltpu.VMEM((hid, vp), jnp.bfloat16),
            pltpu.VMEM((n_blocks, rows, hid), jnp.bfloat16),
            pltpu.VMEM((n_blocks,) + labels.shape, jnp.int32),
            pltpu.VMEM((2, rows, vp), jnp.float32),
            pltpu.VMEM((2, hid, rows), jnp.bfloat16),
        ] + [pltpu.VMEM((2, rows, LANES), jnp.float32)] * 3 + [
            pltpu.VMEM((2, rows, LANES), jnp.int32),
            dma((3,)), dma((2,)), dma((2,)),
        ] + [dma((4,))] * 8 + [dma((8,))] * 2 + [dma((16,))] * 2,
        compiler_params=pltpu.CompilerParams(collective_id=0, has_side_effects=True, vmem_limit_bytes=VMEM_LIMIT),
        name="front",
    )(w_pad, hidden, labels)


def _stats_kernel(st_ref, o_ref, got, s1, r1, s2, r2):
    n, n_z = 16, 4
    dp, zi, tp = lax.axis_index("dp"), lax.axis_index("fsdp"), lax.axis_index("tp")
    me = tp * n_z + zi

    def dev(p):
        return (dp, lax.rem(p, n_z), lax.div(p, n_z))

    peers = [lax.rem(me + o, n) for o in range(n)]
    barrier = pltpu.get_barrier_semaphore()
    for o in range(1, n):
        pl.semaphore_signal(barrier, inc=1, device_id=dev(peers[o]), device_id_type=MESH)
    pl.semaphore_wait(barrier, n - 1)
    first = [
        pltpu.make_async_remote_copy(st_ref.at[peers[o]], got.at[o], s1.at[o], r1.at[o], device_id=dev(peers[o]), device_id_type=MESH)
        for o in range(1, n)
    ]
    for copy in first:
        copy.start()
    got[0] = st_ref[me]
    for copy in first:
        copy.wait_recv()
    parts = [got[o] for o in range(n)]
    m_row = parts[0][0:1]
    for p in parts[1:]:
        m_row = jnp.maximum(m_row, p[0:1])
    s_row = jnp.zeros_like(m_row)
    t_row = jnp.zeros_like(m_row)
    for p in parts:
        s_row = s_row + p[1:2] * jnp.exp(p[0:1] - m_row)
        t_row = t_row + p[2:3]
    loss = m_row + jnp.log(s_row) - t_row
    o_ref[me] = jnp.concatenate([m_row, 1.0 / s_row, loss, m_row], axis=0)
    second = [
        pltpu.make_async_remote_copy(o_ref.at[me], o_ref.at[me], s2.at[o], r2.at[o], device_id=dev(peers[o]), device_id_type=MESH)
        for o in range(1, n)
    ]
    for copy in first:
        copy.wait_send()
    for copy in second:
        copy.start()
    for copy in second:
        copy.wait()


def _stats_call(st):
    n = st.shape[0]
    vmem = pl.BlockSpec(memory_space=pltpu.VMEM)
    return pl.pallas_call(
        _stats_kernel,
        in_specs=[vmem],
        out_specs=vmem,
        out_shape=jax.ShapeDtypeStruct(st.shape, jnp.float32),
        scratch_shapes=[pltpu.VMEM(st.shape, jnp.float32)] + [pltpu.SemaphoreType.DMA((n,))] * 4,
        compiler_params=pltpu.CompilerParams(collective_id=1, has_side_effects=True),
        name="stats",
    )(st)


def _grad_call(c, ids, z, w, st, lab, g_all, v0, sub):
    n_blocks, rows, vp = z.shape
    hid = w.shape[0]
    nb = 4
    tokens = n_blocks * rows
    extra = [] if g_all is None else list(g_all)

    def tp_of(i, ids):
        core = lax.rem(ids[0] + 1 + lax.div(i, 2), 2)
        y = lax.rem(ids[1] + lax.rem(i, 2), 2)
        return y * 2 + core

    def at(i, ids):
        return (tp_of(i, ids), c, 0)

    def at_row(i, ids):
        return (tp_of(i, ids), 0, c)

    return pl.pallas_call(
        functools.partial(_grad_kernel, v0, 1.0 / tokens),
        grid_spec=pltpu.PrefetchScalarGridSpec(
            num_scalar_prefetch=1,
            grid=(n_blocks // nb,),
            in_specs=[
                pl.BlockSpec((nb, sub, vp), at),
                pl.BlockSpec((hid, vp), lambda i, ids: (0, 0)),
                pl.BlockSpec((nb, STATS, sub), at_row),
                pl.BlockSpec((nb, 8, sub), at_row),
            ] + [pl.BlockSpec(memory_space=pl.ANY)] * len(extra),
            out_specs=[
                pl.BlockSpec((nb, sub, v0), at),
                pl.BlockSpec((nb, sub, vp - v0), at),
                pl.BlockSpec((1, nb, sub, hid), lambda i, ids: (lax.max(i - 2, 0), 0, 0, 0)),
                pl.BlockSpec((1, nb, sub, hid), lambda i, ids: (lax.min(i, 1), 0, 0, 0)),
            ],
        ),
        out_shape=[
            jax.ShapeDtypeStruct((n_blocks, rows, v0), jnp.bfloat16),
            jax.ShapeDtypeStruct((n_blocks, rows, vp - v0), jnp.bfloat16),
            jax.ShapeDtypeStruct((2, nb, sub, hid), jnp.float32),
            jax.ShapeDtypeStruct((2, nb, sub, hid), jnp.float32),
        ],
        input_output_aliases={5: 0, 6: 1} if extra else {},
        compiler_params=pltpu.CompilerParams(vmem_limit_bytes=VMEM_LIMIT),
        cost_estimate=pl.CostEstimate(flops=2 * n_blocks * sub * hid * vp, bytes_accessed=n_blocks * sub * vp * 6, transcendentals=n_blocks * sub * vp),
        name="grad_dx",
    )(ids, z, w, st, lab, *extra)


def _dw_call(xt, g, width, col=0):
    hid, tokens = xt.shape
    sub = g.shape[1]
    kb = 1024
    steps = tokens // kb
    return pl.pallas_call(
        functools.partial(_dw_kernel, steps),
        grid=(steps,),
        in_specs=[
            pl.BlockSpec((hid, kb), lambda k: (0, k)),
            pl.BlockSpec((kb // sub, sub, width), lambda k: (k, 0, col)),
        ],
        out_specs=pl.BlockSpec((hid, width), lambda k: (0, 0)),
        out_shape=jax.ShapeDtypeStruct((hid, width), jnp.bfloat16),
        scratch_shapes=[pltpu.VMEM((hid, width), jnp.float32)],
        compiler_params=pltpu.CompilerParams(vmem_limit_bytes=VMEM_LIMIT),
        cost_estimate=pl.CostEstimate(flops=2 * tokens * hid * width, bytes_accessed=tokens * (width + hid) * 2, transcendentals=0),
        name="dw",
    )(xt, g)


def _place_kernel(n_z, edges, zi_ref, *refs):
    o_ref = refs[-1]
    j = pl.program_id(0)
    dist = lax.rem(zi_ref[0] + n_z - j, n_z)
    for s in range(n_z):
        @pl.when(dist == s)
        def _():
            for m, (c0, c1) in enumerate(edges):
                o_ref[:, c0:c1] = refs[len(edges) * s + m][...]


def _place_call(zi, pieces, n_z, vp, vocab_dev):
    rows = pieces[0].shape[0]
    edges, c0 = [], 0
    for p in pieces[:len(pieces) // n_z]:
        edges.append((c0, c0 + p.shape[1]))
        c0 += p.shape[1]
    return pl.pallas_call(
        functools.partial(_place_kernel, n_z, edges),
        grid=(n_z,),
        in_specs=[pl.BlockSpec(memory_space=pltpu.SMEM)]
        + [pl.BlockSpec(p.shape, lambda j: (0, 0)) for p in pieces],
        out_specs=pl.BlockSpec((rows, vp), lambda j: (0, j)),
        out_shape=jax.ShapeDtypeStruct((rows, vocab_dev), jnp.bfloat16),
        compiler_params=pltpu.CompilerParams(vmem_limit_bytes=VMEM_LIMIT),
        name="place",
    )(zi, *pieces)


def _after(value, *deps):
    return lax.optimization_barrier((value,) + deps)[0]


def solution(mesh):
    n_z = mesh.shape["fsdp"]
    n_tp = mesh.shape["tp"]
    n_blocks = n_z * n_tp
    token_spec = P(("dp", "fsdp", "tp"), None)
    label_spec = P(("dp", "fsdp", "tp"))

    def z_shift(a, s):
        return lax.ppermute(a, "fsdp", [(k, (k + s) % n_z) for k in range(n_z)])

    def swap(a, axis, bit):
        return lax.ppermute(a, axis, [(k, k ^ bit) for k in range(mesh.shape[axis])])

    def pick(a, i, axis=0):
        return lax.dynamic_index_in_dim(a, i, axis, keepdims=False)

    def step(hidden, w_head, labels):
        rows_dev, hid = hidden.shape
        w_rows, vocab_dev = w_head.shape
        tokens = rows_dev * n_blocks
        vp = _ceil_to(-(-vocab_dev // n_z), LANES)
        sub = rows_dev // CHUNKS
        zi = lax.axis_index("fsdp")
        tpi = lax.axis_index("tp")
        yi, ci = tpi // 2, tpi % 2

        w_pad = jnp.pad(w_head, ((0, 0), (0, n_z * vp - vocab_dev)))
        w_full, lab, z_all, xt, local = _front_call(w_pad, hidden, labels.reshape(1, rows_dev), vp, vocab_dev, n_blocks)

        lab = lab - (tpi * vocab_dev + zi * vp)
        valid = jnp.minimum(vocab_dev - zi * vp, vp).astype(jnp.int32)
        lab = jnp.where((lab >= 0) & (lab < valid), lab, -1 - 2 * LANES).astype(jnp.float32)
        lab = jnp.broadcast_to(lab, (n_blocks, 8, rows_dev))

        st = _stats_call(local)
        mean_loss = (jnp.sum(st[:, 2]) * (1.0 / tokens)).reshape(1)

        v0 = _tiles(vp)[2][0]
        ids = jnp.stack([ci, yi]).astype(jnp.int32)

        def grad(c, g_all, *deps):
            i = _after(ids, *deps) if deps else ids
            g0, g1, keep, send = _grad_call(c, i, z_all, w_full, st, lab, g_all, v0, sub)
            return (g0, g1), keep, swap(send, "tp", 1)

        def to_y(c, *deps):
            keep = _after(keeps[c], *deps)
            other = keep[1] + gots[c][1]
            mine = keep[0] + gots[c][0]
            ys[c] = (mine, swap(other, "tp", 2))
            return mine, other

        def to_near(c, *deps):
            both = (_after(ys[c][0], *deps) + ys[c][1]).reshape(2, 2, sub, hid)
            odd = zi % 2
            mine, other = pick(both, odd, 1), pick(both, 1 - odd, 1)
            nears[c] = (mine, swap(other, "fsdp", 1))
            return mine, other

        def to_far(c, *deps):
            both = _after(nears[c][0], *deps) + nears[c][1]
            high = zi // 2
            mine, other = pick(both, high), pick(both, 1 - high)
            fars[c] = (mine, swap(other, "fsdp", 2))
            return mine, other

        def last(c, *deps):
            return (_after(fars[c][0], *deps) + fars[c][1]).astype(jnp.bfloat16)

        def send_dw(dw):
            parts = [pick(dw, (zi + s) % n_z) for s in range(n_z)]
            sent = [parts[0]]
            for s in range(1, n_z):
                sent.append(z_shift(parts[s], s))
            return parts, sent

        def wide_near(c, *deps):
            both = (_after(keeps[c], *deps) + gots[c]).reshape(2, 2, 2, sub, hid)
            odd = zi % 2
            mine, other = pick(both, odd, 2), pick(both, 1 - odd, 2)
            nears[c] = (mine, swap(other, "fsdp", 1))
            return mine, other

        def wide_far(c, *deps):
            both = _after(nears[c][0], *deps) + nears[c][1]
            high = zi // 2
            mine, other = pick(both, high, 1), pick(both, 1 - high, 1)
            fars[c] = (mine, swap(other, "fsdp", 2))
            return mine, other

        def wide_y(c, *deps):
            both = _after(fars[c][0], *deps) + fars[c][1]
            fars[c] = (both[0], swap(both[1], "tp", 2))
            return (both,)

        keeps, gots, ys, nears, fars = ([None] * CHUNKS for _ in range(5))
        g, keeps[0], gots[0] = grad(0, None)
        g, keeps[1], gots[1] = grad(1, g, keeps[0])
        t = wide_near(0, keeps[1])
        g, keeps[2], gots[2] = grad(2, g, *t)
        t = to_y(1, keeps[2])
        g, keeps[3], gots[3] = grad(3, g, *t)
        t = to_y(2, keeps[3])
        vh = v0 // 2
        dwa = _dw_call(_after(xt, *t), g[0], vh, 0).reshape(n_z, w_rows, vh)
        partsa, piecesa = send_dw(dwa)
        t = wide_far(0, dwa) + tuple(partsa)
        dw0 = _dw_call(_after(xt, *t), g[0], vh, 1).reshape(n_z, w_rows, vh)
        parts0, pieces0 = send_dw(dw0)
        t = to_near(1, dw0) + to_y(3, dw0) + wide_y(0, dw0) + tuple(parts0)
        dw1 = _dw_call(_after(xt, *t), g[1], vp - v0).reshape(n_z, w_rows, vp - v0)
        parts1, pieces1 = send_dw(dw1)
        t = to_near(2, *parts1)
        t = to_far(1, *t)
        t = to_near(3, *t)
        t = to_far(2, *t)
        t = to_far(3, *t)
        out = [last(c, *t) for c in range(CHUNKS)]
        pieces = [p for group in zip(piecesa, pieces0, pieces1) for p in group]
        zv = _after(zi.reshape(1).astype(jnp.int32), *out)
        d_w = _place_call(zv, pieces, n_z, vp, vocab_dev)
        return mean_loss, jnp.concatenate(out, axis=0), d_w

    return jax.shard_map(
        step,
        mesh=mesh,
        in_specs=(token_spec, P("fsdp", "tp"), label_spec),
        out_specs=(P("dp"), token_spec, P(("dp", "fsdp"), "tp")),
        check_vma=False,
    )
```
